256 devices in a mesh: rows: 32 (over x, z), tensor: 2 (over core), groups: 4 (over y).
Axes of the slice: x: 4, y: 4, z: 8, core: 2. Of those that a mesh axis runs over, the one named last changes fastest.
Arguments:
- effects: float32 [32768, 1024], P(('groups', 'rows'), 'tensor'), parts along dimension 0, may hold values from -8 to 8
Outputs:
- basis: float32 [32768, 1024], P(('groups', 'rows'), 'tensor'), parts along dimension 0
- triangle: float32 [4096, 1024], P('groups', 'tensor'), parts along dimension 0
The draws below stay inside these ranges and needn't reach their ends.
There are 4 independent parts, one for each index of `groups`. The reference program is written for one: setup_inputs(seed, part) draws one part's arguments, and reference() takes and returns one part's arrays. A program takes and returns all parts, laid end to end along the dimension named above; each array names one. Nothing has to cross between parts.
All inputs are finite; a program needn't handle non-finite values.
Results may differ from the reference program's by a relative error of at most 0.000075.
Values sent between devices are 32-bit elements; how exact they have to be, the bound alone decides.
A program may use at most 64 MiB of HBM per device.

```python
import jax
import jax.numpy as jnp
from jax import lax

COLS = 1024
ROWS = 8192


def block_levels(rng, dims, split, smallest, largest):
    loudness = 1.0
    for axis_at, parts in split:
        steps = jax.random.uniform(jax.random.fold_in(jax.random.fold_in(rng, 6), axis_at), (parts,), jnp.float32, smallest / len(split), largest / len(split))
        loudness = loudness * jnp.repeat(jnp.exp(steps), dims[axis_at] // parts).reshape((-1,) + (1,) * (len(dims) - 1 - axis_at))
    return loudness


def gaussian(own_key, extent, deviation, reach, cuts=(), dtype=jnp.bfloat16):
    result = jax.random.normal(own_key, extent, jnp.float32) * deviation
    if len(cuts) > 0:
        result = block_levels(own_key, extent, cuts, -0.22, 0.18) * result
    return jnp.clip(result, min=-reach, max=reach).astype(dtype)


def setup_inputs(seed: int = 0, part: int = 0) -> dict:
    arg_keys = jax.random.split(jax.random.key(seed), 2)
    own_keys = jax.random.split(jax.random.fold_in(arg_keys[1], part), 2)
    return {
        "effects": gaussian(own_keys[0], (ROWS, COLS), 1.0, 8.0, ((0, 32), (1, 2)), jnp.float32),
    }


def reference(effects):
    gram = jnp.dot(effects.T.astype(jnp.float32), effects.astype(jnp.float32), precision=lax.Precision.HIGHEST, preferred_element_type=jnp.float32)
    lower = jnp.linalg.cholesky(gram)
    total = effects.shape[0]
    solved = lax.linalg.triangular_solve(lower, effects, left_side=False, lower=True, transpose_a=True)
    basis = solved * jnp.sqrt(jnp.float32(total))
    triangle = lower.T / jnp.sqrt(jnp.float32(total))
    return (basis, triangle)
```

```python
import jax
import jax.numpy as jnp
from jax import lax
from jax.experimental import pallas as pl
from jax.experimental.pallas import tpu as pltpu
from jax.sharding import PartitionSpec as P

f32 = jnp.float32
bf16 = jnp.bfloat16
BLOCK = 128
BASE = 32


def split3(x):
    high = x.astype(bf16)
    rest = x - high.astype(f32)
    middle = rest.astype(bf16)
    return high, middle, (rest - middle.astype(f32)).astype(bf16)


def left(parts, dim):
    h, m, l = parts
    return jnp.concatenate([h, h, m, h, m, l], dim)


def right(parts, dim):
    h, m, l = parts
    return jnp.concatenate([h, m, h, l, m, h], dim)


def dot_over(a, b, dim):
    return lax.dot_general(a, b, (((dim,), (dim,)), ((), ())), preferred_element_type=f32)


def eliminate(rows, offset):
    tiles = BASE // 8
    cols = [
        [
            jnp.broadcast_to(rows[8 * t : 8 * t + 8, offset + j : offset + j + 1], (8, BLOCK))
            for t in range(tiles)
        ]
        for j in range(BASE)
    ]
    panel = [
        [rows[8 * t : 8 * t + 8, BLOCK * c : BLOCK * (c + 1)] for c in range(2)]
        for t in range(tiles)
    ]
    row = lax.broadcasted_iota(jnp.int32, (8, BLOCK), 0)
    scales = [jnp.zeros((8, BLOCK), f32) for _ in range(tiles)]
    for j in range(BASE):
        t0, r = divmod(j, 8)
        inv = lax.rsqrt(jnp.broadcast_to(cols[j][t0][r : r + 1], (8, BLOCK)))
        scales[t0] = jnp.where(row == r, inv, scales[t0])
        column = [cols[j][t] * inv for t in range(t0, tiles)]
        below = [jnp.where(row > r, column[0], 0.0)] + column[1:]
        pivot = [jnp.broadcast_to(panel[t0][c][r : r + 1], (8, BLOCK)) * inv for c in range(2)]
        for t in range(t0, tiles):
            for c in range(2):
                panel[t][c] = panel[t][c] - below[t - t0] * pivot[c]
        for j2 in range(j + 1, BASE):
            t2, r2 = divmod(j2, 8)
            factor = jnp.broadcast_to(column[t2 - t0][r2 : r2 + 1], (8, BLOCK))
            for t in range(t2, tiles):
                cols[j2][t] = cols[j2][t] - column[t - t0] * factor
    return jnp.concatenate(
        [jnp.concatenate([panel[t][c] * scales[t] for c in range(2)], 1) for t in range(tiles)], 0
    )


def factor_block(block):
    shape = (BLOCK, BLOCK)
    row = lax.broadcasted_iota(jnp.int32, shape, 0)
    col = lax.broadcasted_iota(jnp.int32, shape, 1)
    rest = jnp.concatenate([block, jnp.where(row == col, 1.0, 0.0).astype(f32)], 1)
    done = []
    for s in range(0, BLOCK, BASE):
        rows = eliminate(rest[:BASE], s)
        at = lax.broadcasted_iota(jnp.int32, rows.shape, 1)
        diag = lax.broadcasted_iota(jnp.int32, rows.shape, 0) + s
        rows = jnp.where(at < jnp.minimum(diag, BLOCK), 0.0, rows)
        done.append(rows)
        if s + BASE < BLOCK:
            update = dot_over(left(split3(rows[:, :BLOCK]), 0), right(split3(rows), 0), 0)
            rest = rest[BASE:] - update[s + BASE :]
    return jnp.concatenate(done, 0)


def factor_kernel(gram_ref, rows_ref, solved_ref, upper_ref, work, lhs, rhs):
    n = gram_ref.shape[0]
    full = n + rows_ref.shape[0]
    work[:n] = gram_ref[...]
    work[n:] = rows_ref[...]
    for c0 in range(0, n, BLOCK):
        c1 = c0 + BLOCK
        if c0:
            upper_ref[c0:c1, :c0] = jnp.zeros((BLOCK, c0), f32)
        factored = factor_block(work[c0:c1, c0:c1])
        upper_ref[c0:c1, c0:c1] = factored[:, :BLOCK]
        inverse = right(split3(factored[:, BLOCK:]), 1)
        for r in range(c1, full, BLOCK):
            solved = dot_over(left(split3(work[r : r + BLOCK, c0:c1]), 1), inverse, 1)
            parts = split3(solved)
            lhs[r : r + BLOCK] = left(parts, 1)
            if r >= n:
                solved_ref[r - n : r - n + BLOCK, c0:c1] = solved
            else:
                upper_ref[c0:c1, r : r + BLOCK] = solved.T
                rhs[r : r + BLOCK] = right(parts, 1)
        j = c1
        while j < n:
            width = BLOCK if (j // BLOCK) % 2 else min(2 * BLOCK, n - j)
            against = rhs[j : j + width]
            for r in range(j, full, 2 * BLOCK):
                h = min(2 * BLOCK, full - r)
                work[r : r + h, j : j + width] -= dot_over(lhs[r : r + h], against, 1)
            j += width


def factor_and_solve(gram, rows):
    n, m = gram.shape[0], rows.shape[0]
    return pl.pallas_call(
        factor_kernel,
        out_shape=[jax.ShapeDtypeStruct((m, n), f32), jax.ShapeDtypeStruct((n, n), f32)],
        scratch_shapes=[
            pltpu.VMEM((n + m, n), f32),
            pltpu.VMEM((n + m, 6 * BLOCK), bf16),
            pltpu.VMEM((n, 6 * BLOCK), bf16),
        ],
        compiler_params=pltpu.CompilerParams(vmem_limit_bytes=60 * 2**20),
    )(gram, rows)


def in_order(parts, dim):
    dims = list(parts.shape[1:])
    dims[dim] *= parts.shape[0]
    return jnp.moveaxis(parts, 0, dim).reshape(dims)


def from_everyone(value, axis):
    size = lax.axis_size(axis)
    return lax.all_to_all(
        jnp.broadcast_to(value[None], (size, *value.shape)), axis, 0, 0, tiled=True
    )


def shards(effects):
    whole = in_order(from_everyone(effects, "tensor"), 1)
    width = effects.shape[1]
    local_gram = jnp.dot(
        whole.T, whole, precision=lax.Precision.HIGHEST, preferred_element_type=jnp.float32
    )
    gram = lax.psum(local_gram, "rows")
    solved, upper = factor_and_solve(gram, whole)
    total = effects.shape[0] * lax.axis_size("rows")
    scale = jnp.sqrt(jnp.float32(total))
    start = lax.axis_index("tensor") * width
    basis = lax.dynamic_slice_in_dim(solved, start, width, 1) * scale
    triangle = lax.dynamic_slice_in_dim(upper, start, width, 1) / scale
    return (basis, triangle)


def solution(mesh):
    in_specs = (P(("groups", "rows"), "tensor"),)
    out_specs = (P(("groups", "rows"), "tensor"), P("groups", "tensor"))
    return jax.shard_map(shards, mesh=mesh, in_specs=in_specs, out_specs=out_specs, check_vma=False)
```

```python
import functools

import jax
import jax.numpy as jnp
from jax import lax
from jax.experimental import pallas as pl
from jax.experimental.pallas import tpu as pltpu
from jax.sharding import PartitionSpec as P

f32 = jnp.float32
bf16 = jnp.bfloat16
BLOCK = 128
BASE = 32


def split3(x):
    high = x.astype(bf16)
    rest = x - high.astype(f32)
    middle = rest.astype(bf16)
    return high, middle, (rest - middle.astype(f32)).astype(bf16)


def left(parts, dim):
    h, m, l = parts
    return jnp.concatenate([h, h, m, h, m, l], dim)


def right(parts, dim):
    h, m, l = parts
    return jnp.concatenate([h, m, h, l, m, h], dim)


def dot_over(a, b, dim):
    return lax.dot_general(a, b, (((dim,), (dim,)), ((), ())), preferred_element_type=f32)


def eliminate(rows, offset):
    tiles = BASE // 8
    cols = [
        [
            jnp.broadcast_to(rows[8 * t : 8 * t + 8, offset + j : offset + j + 1], (8, BLOCK))
            for t in range(tiles)
        ]
        for j in range(BASE)
    ]
    panel = [
        [rows[8 * t : 8 * t + 8, BLOCK * c : BLOCK * (c + 1)] for c in range(2)]
        for t in range(tiles)
    ]
    row = lax.broadcasted_iota(jnp.int32, (8, BLOCK), 0)
    scales = [jnp.zeros((8, BLOCK), f32) for _ in range(tiles)]
    for j in range(BASE):
        t0, r = divmod(j, 8)
        inv = lax.rsqrt(jnp.broadcast_to(cols[j][t0][r : r + 1], (8, BLOCK)))
        scales[t0] = jnp.where(row == r, inv, scales[t0])
        column = [cols[j][t] * inv for t in range(t0, tiles)]
        below = [jnp.where(row > r, column[0], 0.0)] + column[1:]
        pivot = [jnp.broadcast_to(panel[t0][c][r : r + 1], (8, BLOCK)) * inv for c in range(2)]
        for t in range(t0, tiles):
            for c in range(2):
                panel[t][c] = panel[t][c] - below[t - t0] * pivot[c]
        for j2 in range(j + 1, BASE):
            t2, r2 = divmod(j2, 8)
            factor = jnp.broadcast_to(column[t2 - t0][r2 : r2 + 1], (8, BLOCK))
            for t in range(t2, tiles):
                cols[j2][t] = cols[j2][t] - column[t - t0] * factor
    return jnp.concatenate(
        [jnp.concatenate([panel[t][c] * scales[t] for c in range(2)], 1) for t in range(tiles)], 0
    )


def factor_block(block):
    shape = (BLOCK, BLOCK)
    row = lax.broadcasted_iota(jnp.int32, shape, 0)
    col = lax.broadcasted_iota(jnp.int32, shape, 1)
    rest = jnp.concatenate([block, jnp.where(row == col, 1.0, 0.0).astype(f32)], 1)
    done = []
    for s in range(0, BLOCK, BASE):
        rows = eliminate(rest[:BASE], s)
        at = lax.broadcasted_iota(jnp.int32, rows.shape, 1)
        diag = lax.broadcasted_iota(jnp.int32, rows.shape, 0) + s
        rows = jnp.where(at < jnp.minimum(diag, BLOCK), 0.0, rows)
        done.append(rows)
        if s + BASE < BLOCK:
            update = dot_over(left(split3(rows[:, :BLOCK]), 0), right(split3(rows), 0), 0)
            rest = rest[BASE:] - update[s + BASE :]
    return jnp.concatenate(done, 0)


def factor_kernel(gram_ref, rows_ref, solved_ref, upper_ref, work, lhs, rhs):
    full, n = work.shape
    for at, (i, j) in enumerate(lower_blocks(n // BLOCK)):
        work[i * BLOCK : (i + 1) * BLOCK, j * BLOCK : (j + 1) * BLOCK] = gram_ref[at]
    work[n:] = rows_ref[...]
    for c0 in range(0, n, BLOCK):
        c1 = c0 + BLOCK
        if c0:
            upper_ref[c0:c1, :c0] = jnp.zeros((BLOCK, c0), f32)
        factored = factor_block(work[c0:c1, c0:c1])
        upper_ref[c0:c1, c0:c1] = factored[:, :BLOCK]
        inverse = right(split3(factored[:, BLOCK:]), 1)
        for r in range(c1, full, BLOCK):
            solved = dot_over(left(split3(work[r : r + BLOCK, c0:c1]), 1), inverse, 1)
            parts = split3(solved)
            lhs[r : r + BLOCK] = left(parts, 1)
            if r >= n:
                solved_ref[r - n : r - n + BLOCK, c0:c1] = solved
            else:
                upper_ref[c0:c1, r : r + BLOCK] = solved.T
                rhs[r : r + BLOCK] = right(parts, 1)
        j = c1
        while j < n:
            width = BLOCK if (j // BLOCK) % 2 else min(2 * BLOCK, n - j)
            against = rhs[j : j + width]
            for r in range(j, full, 2 * BLOCK):
                h = min(2 * BLOCK, full - r)
                work[r : r + h, j : j + width] -= dot_over(lhs[r : r + h], against, 1)
            j += width


def factor_and_solve(gram, rows):
    m, n = rows.shape
    return pl.pallas_call(
        factor_kernel,
        out_shape=[jax.ShapeDtypeStruct((m, n), f32), jax.ShapeDtypeStruct((n, n), f32)],
        scratch_shapes=[
            pltpu.VMEM((n + m, n), f32),
            pltpu.VMEM((n + m, 6 * BLOCK), bf16),
            pltpu.VMEM((n, 6 * BLOCK), bf16),
        ],
        compiler_params=pltpu.CompilerParams(vmem_limit_bytes=60 * 2**20),
    )(gram, rows)


CHUNK_BLOCKS = (4, 4, 4, 4, 2)


def lower_blocks(count):
    return [(i, j) for j in range(count) for i in range(j, count)]


def remote(src, dst, send, recv, place):
    return pltpu.make_async_remote_copy(
        src_ref=src,
        dst_ref=dst,
        send_sem=send,
        recv_sem=recv,
        device_id=place,
        device_id_type=pl.DeviceIdType.MESH,
    )


def gram_kernel(nx, nz, mine_ref, gram_ref, whole_ref, lhs, rhs, part, in_f, in_s, in_z,
                swap_sems, pair_sems, z_send, z_recv, g_send, g_recv):
    rows_id = lax.axis_index("rows")
    core = lax.axis_index("tensor")
    x, z = rows_id // nz, rows_id % nz
    near = x + 1 - 2 * (x % 2)
    far = nx - 1 - x
    high = x // 2
    low = (high + x % 2) % 2
    first = (1 - core) * near + core * far
    second = (1 - core) * far + core * near
    bit_f = (1 - core) * low + core * high
    bit_s = (1 - core) * high + core * low
    to_core = {"rows": rows_id, "tensor": 1 - core}
    to_first = {"rows": first * nz + z, "tensor": core}
    to_second = {"rows": second * nz + z, "tensor": core}

    def to_z(step):
        return {"rows": x * nz + (z + step) % nz, "tensor": core}

    barrier = pltpu.get_barrier_semaphore()
    places = [to_core, to_first, to_second] + [to_z(s) for s in range(1, nz)]
    for place in places:
        pl.semaphore_signal(
            barrier, inc=1, device_id=place, device_id_type=pl.DeviceIdType.MESH
        )
    pl.semaphore_wait(barrier, len(places))

    m, width = mine_ref.shape
    own = pl.ds(pl.multiple_of(core * width, width), width)
    swap = remote(mine_ref, whole_ref.at[:, own], swap_sems.at[0], swap_sems.at[1], to_core)
    swap.start()
    whole_ref[:, own] = mine_ref[...]
    swap.wait()
    for c in range(0, 2 * width, BLOCK):
        parts = split3(whole_ref[:, c : c + BLOCK].T)
        lhs[c : c + BLOCK] = left(parts, 1)
        rhs[c : c + BLOCK] = right(parts, 1)

    blocks = lower_blocks(2 * width // BLOCK)
    starts = [sum(CHUNK_BLOCKS[:i]) for i in range(len(CHUNK_BLOCKS) + 1)]

    def base_of(i):
        return 2 * starts[i] + core * CHUNK_BLOCKS[i]

    def quarter(i, ref, at, which):
        n = CHUNK_BLOCKS[i]
        if n == 4:
            return ref.at[at + which]
        half = BLOCK // 2
        return ref.at[at + which // 2, pl.ds(pl.multiple_of((which % 2) * half, half), half)]

    def half(i, ref, at, which):
        n = CHUNK_BLOCKS[i] // 2
        return ref.at[pl.ds(at + n * which, n)]

    def piece(i, view, index):
        n = CHUNK_BLOCKS[i] * BLOCK // (nx * nz)
        return view.at[pl.ds(pl.multiple_of(index * n, n), n)]

    def copy_first(i):
        return remote(
            half(i, part, starts[i], 1 - bit_f), half(i, in_f, starts[i] // 2, 0),
            pair_sems.at[i, 0], pair_sems.at[i, 1], to_first)

    def arrived(i, ref, which):
        return ref.at[i] if CHUNK_BLOCKS[i] == 4 else ref.at[i, pl.ds(0, BLOCK // 2)]

    def copy_second(i):
        return remote(
            quarter(i, part, starts[i], 2 * bit_f + 1 - bit_s), arrived(i, in_s, 0),
            pair_sems.at[i, 2], pair_sems.at[i, 3], to_second)

    def own_part(i):
        return quarter(i, part, starts[i], 2 * bit_f + bit_s)

    def own_gram(i):
        return quarter(i, gram_ref, base_of(i), 2 * bit_f + bit_s)

    def in_piece(i, index):
        n = CHUNK_BLOCKS[i] * BLOCK // (nx * nz)
        return in_z.at[i, index, pl.ds(0, n)]

    def copy_z(i, step):
        return remote(
            piece(i, own_part(i), (z + step) % nz), in_piece(i, nz - step),
            z_send.at[i, step], z_recv.at[i, nz - step], to_z(step))

    def copy_z_in(i, step):
        return remote(
            piece(i, own_part(i), z), in_piece(i, step),
            z_send.at[i, step], z_recv.at[i, step], to_z(step))

    def copy_gather(i, step):
        mine = piece(i, own_gram(i), z)
        return remote(mine, mine, g_send.at[i, step], g_recv.at[i, nz - step], to_z(step))

    def copy_gather_in(i, step):
        theirs = piece(i, own_gram(i), (z + step) % nz)
        return remote(theirs, theirs, g_send.at[i, step], g_recv.at[i, step], to_z(step))

    def copy_back_second(i, bit):
        view = quarter(i, gram_ref, base_of(i), 2 * bit_f + bit)
        return remote(view, view, pair_sems.at[i, 4], pair_sems.at[i, 5], to_second)

    def copy_back_first(i, bit):
        view = half(i, gram_ref, base_of(i), bit)
        return remote(view, view, pair_sems.at[i, 6], pair_sems.at[i, 7], to_first)

    def copy_core(i, side):
        view = gram_ref.at[pl.ds(2 * starts[i] + side * CHUNK_BLOCKS[i], CHUNK_BLOCKS[i])]
        return remote(view, view, pair_sems.at[i, 8], pair_sems.at[i, 9], to_core)

    def stage_gram(i):
        for q in range(CHUNK_BLOCKS[i]):
            a, b = blocks[2 * starts[i] + q], blocks[2 * starts[i] + CHUNK_BLOCKS[i] + q]
            bi = pl.multiple_of((a[0] + core * (b[0] - a[0])) * BLOCK, BLOCK)
            bj = pl.multiple_of((a[1] + core * (b[1] - a[1])) * BLOCK, BLOCK)
            part[starts[i] + q] = dot_over(lhs[pl.ds(bi, BLOCK)], rhs[pl.ds(bj, BLOCK)], 1)
        copy_first(i).start()

    def stage_first(i):
        copy_first(i).wait()
        n = CHUNK_BLOCKS[i] // 2
        at = pl.ds(starts[i] + n * bit_f, n)
        part[at] += in_f[pl.ds(starts[i] // 2, n)]
        copy_second(i).start()

    def stage_second(i):
        copy_second(i).wait()
        mine = own_part(i)
        mine[...] += arrived(i, in_s, 0)[...]
        for step in range(1, nz):
            copy_z(i, step).start()

    def stage_scatter(i):
        total = piece(i, own_part(i), z)[...]
        for step in range(1, nz):
            copy_z_in(i, step).wait_recv()
            total = total + in_piece(i, step)[...]
        piece(i, own_gram(i), z)[...] = total
        for step in range(1, nz):
            copy_gather(i, step).start()

    def stage_gather(i):
        for step in range(1, nz):
            copy_gather_in(i, step).wait_recv()
        copy_back_second(i, bit_s).start()

    def stage_back_second(i):
        copy_back_second(i, 1 - bit_s).wait_recv()
        copy_back_first(i, bit_f).start()

    def stage_back_first(i):
        copy_back_first(i, 1 - bit_f).wait_recv()
        copy_core(i, core).start()

    def stage_core(i):
        copy_core(i, 1 - core).wait_recv()

    stages = (stage_gram, stage_first, stage_second, stage_scatter, stage_gather,
              stage_back_second, stage_back_first, stage_core)
    chunks = len(CHUNK_BLOCKS)
    for t in range(chunks + len(stages) - 1):
        for s in reversed(range(len(stages))):
            if 0 <= t - s < chunks:
                stages[s](t - s)
    for i in range(chunks):
        for step in range(1, nz):
            copy_z(i, step).wait_send()
            copy_gather(i, step).wait_send()
        copy_back_second(i, bit_s).wait_send()
        copy_back_first(i, bit_f).wait_send()
        copy_core(i, core).wait_send()


def reduced_gram(mine, nx, nz):
    m, width = mine.shape
    n = 2 * width
    count = len(lower_blocks(n // BLOCK))
    chunks = len(CHUNK_BLOCKS)
    dma = pltpu.SemaphoreType.DMA
    return pl.pallas_call(
        functools.partial(gram_kernel, nx, nz),
        out_shape=[
            jax.ShapeDtypeStruct((count, BLOCK, BLOCK), f32),
            jax.ShapeDtypeStruct((m, n), f32),
        ],
        in_specs=[pl.BlockSpec(memory_space=pltpu.VMEM)],
        out_specs=[pl.BlockSpec(memory_space=pltpu.VMEM)] * 2,
        scratch_shapes=[
            pltpu.VMEM((n, 6 * m), bf16),
            pltpu.VMEM((n, 6 * m), bf16),
            pltpu.VMEM((count // 2, BLOCK, BLOCK), f32),
            pltpu.VMEM((count // 4, BLOCK, BLOCK), f32),
            pltpu.VMEM((chunks, BLOCK, BLOCK), f32),
            pltpu.VMEM((chunks, nz, 16, BLOCK), f32),
            dma((2,)),
            dma((chunks, 10)),
            dma((chunks, nz)),
            dma((chunks, nz)),
            dma((chunks, nz)),
            dma((chunks, nz)),
        ],
        compiler_params=pltpu.CompilerParams(
            collective_id=0, has_side_effects=True, vmem_limit_bytes=60 * 2**20
        ),
    )(mine)


def shards(effects):
    nx, nz = 4, lax.axis_size("rows") // 4
    gram, whole = reduced_gram(effects, nx, nz)
    solved, upper = factor_and_solve(gram, whole)
    width = effects.shape[1]
    total = effects.shape[0] * lax.axis_size("rows")
    scale = jnp.sqrt(jnp.float32(total))
    start = lax.axis_index("tensor") * width
    basis = lax.dynamic_slice_in_dim(solved, start, width, 1) * scale
    triangle = lax.dynamic_slice_in_dim(upper, start, width, 1) / scale
    return (basis, triangle)


def solution(mesh):
    in_specs = (P(("groups", "rows"), "tensor"),)
    out_specs = (P(("groups", "rows"), "tensor"), P("groups", "tensor"))
    return jax.shard_map(shards, mesh=mesh, in_specs=in_specs, out_specs=out_specs, check_vma=False)
```

```python
import functools

import jax
import jax.numpy as jnp
from jax import lax
from jax.experimental import pallas as pl
from jax.experimental.pallas import tpu as pltpu
from jax.sharding import PartitionSpec as P

f32 = jnp.float32
bf16 = jnp.bfloat16
BLOCK = 128
BASE = 32


def split3(x):
    high = x.astype(bf16)
    rest = x - high.astype(f32)
    middle = rest.astype(bf16)
    return high, middle, (rest - middle.astype(f32)).astype(bf16)


def left(parts, dim):
    h, m, l = parts
    return jnp.concatenate([h, h, m, h, m, l], dim)


def right(parts, dim):
    h, m, l = parts
    return jnp.concatenate([h, m, h, l, m, h], dim)


def dot_over(a, b, dim):
    return lax.dot_general(a, b, (((dim,), (dim,)), ((), ())), preferred_element_type=f32)


def eliminate(rows, offset):
    tiles = BASE // 8
    cols = [
        [
            jnp.broadcast_to(rows[8 * t : 8 * t + 8, offset + j : offset + j + 1], (8, BLOCK))
            for t in range(tiles)
        ]
        for j in range(BASE)
    ]
    panel = [
        [rows[8 * t : 8 * t + 8, BLOCK * c : BLOCK * (c + 1)] for c in range(2)]
        for t in range(tiles)
    ]
    row = lax.broadcasted_iota(jnp.int32, (8, BLOCK), 0)
    scales = [jnp.zeros((8, BLOCK), f32) for _ in range(tiles)]
    for j in range(BASE):
        t0, r = divmod(j, 8)
        inv = lax.rsqrt(jnp.broadcast_to(cols[j][t0][r : r + 1], (8, BLOCK)))
        scales[t0] = jnp.where(row == r, inv, scales[t0])
        column = [cols[j][t] * inv for t in range(t0, tiles)]
        below = [jnp.where(row > r, column[0], 0.0)] + column[1:]
        pivot = [jnp.broadcast_to(panel[t0][c][r : r + 1], (8, BLOCK)) * inv for c in range(2)]
        for t in range(t0, tiles):
            for c in range(2):
                panel[t][c] = panel[t][c] - below[t - t0] * pivot[c]
        for j2 in range(j + 1, BASE):
            t2, r2 = divmod(j2, 8)
            factor = jnp.broadcast_to(column[t2 - t0][r2 : r2 + 1], (8, BLOCK))
            for t in range(t2, tiles):
                cols[j2][t] = cols[j2][t] - column[t - t0] * factor
    return jnp.concatenate(
        [jnp.concatenate([panel[t][c] * scales[t] for c in range(2)], 1) for t in range(tiles)], 0
    )


def factor_block(block):
    shape = (BLOCK, BLOCK)
    row = lax.broadcasted_iota(jnp.int32, shape, 0)
    col = lax.broadcasted_iota(jnp.int32, shape, 1)
    rest = jnp.concatenate([block, jnp.where(row == col, 1.0, 0.0).astype(f32)], 1)
    done = []
    for s in range(0, BLOCK, BASE):
        rows = eliminate(rest[:BASE], s)
        at = lax.broadcasted_iota(jnp.int32, rows.shape, 1)
        diag = lax.broadcasted_iota(jnp.int32, rows.shape, 0) + s
        rows = jnp.where(at < jnp.minimum(diag, BLOCK), 0.0, rows)
        done.append(rows)
        if s + BASE < BLOCK:
            update = dot_over(left(split3(rows[:, :BLOCK]), 0), right(split3(rows), 0), 0)
            rest = rest[BASE:] - update[s + BASE :]
        yield
    return jnp.concatenate(done, 0)


def factor_steps(work, lhs, rhs, n, base, first, last, put_upper, put_solved):
    full = work.shape[0] + base
    for c0 in range(first, last, BLOCK):
        yield c0
        c1 = c0 + BLOCK
        cols = slice(c0 - base, c1 - base)
        factored = yield from factor_block(work[cols, cols])
        put_upper(c0, c0, factored[:, :BLOCK])
        inverse = right(split3(factored[:, BLOCK:]), 1)
        for r in range(c1, full, BLOCK):
            at = slice(r - base, r - base + BLOCK)
            solved = dot_over(left(split3(work[at, cols]), 1), inverse, 1)
            parts = split3(solved)
            lhs[at] = left(parts, 1)
            if r >= n:
                put_solved(r - n, c0, solved)
            else:
                put_upper(c0, r, solved.T)
                rhs[at] = right(parts, 1)
        yield
        j = c1
        while j < n:
            width = BLOCK if (j // BLOCK) % 2 else min(2 * BLOCK, n - j)
            to = slice(j - base, j - base + width)
            against = rhs[to]
            spans = [(r, min(2 * BLOCK, n - r)) for r in range(j, n, 2 * BLOCK)]
            spans += [(r, min(2 * BLOCK, full - r)) for r in range(n, full, 2 * BLOCK)]
            for r, h in spans:
                at = slice(r - base, r - base + h)
                product = dot_over(lhs[at], against, 1)
                if c0 == 0 and r < n:
                    work[at, to] = -product
                else:
                    work[at, to] -= product
            j += width
            yield


CHUNK_BLOCKS = (4, 4, 4, 4, 2)
CHUNK_STARTS = (0, 2.5, 5, 7.5, 10)
STAGE_TIMES = (
    ("S", 2.9, 0.37),
    ("Z", 2.0, 0.18),
    ("A", 2.8, 0.4),
    ("B", 4.6, 0.4),
    ("C", 3.1, 0.18),
    ("D", 2.6, 0.37),
    ("E", 1.2, 0.1),
    ("W", 0.1, 0.0),
)
FRONT_STEPS = 6
PACE = 1


def stage_order():
    timed = [(0.0, 1, "P", c) for c in range(4)]
    for i, (start, n) in enumerate(zip(CHUNK_STARTS, CHUNK_BLOCKS)):
        timed.append((start - 1.0, 2 if i else 0, "G", i))
        timed.append((start - 1.0 if i == 0 else start, 3 if i else 0, "F", i))
        at = start
        for name, fixed, each in STAGE_TIMES:
            at += fixed + each * n
            timed.append((at, 4 + i, name, i))
    first = [("P", 0)]
    return first + [e[2:] for e in sorted(timed, key=lambda e: e[:2]) if e[2:] != first[0]]


def lower_blocks(count):
    return [(i, j) for j in range(count) for i in range(j, count)]


def remote(src, dst, send, recv, place):
    return pltpu.make_async_remote_copy(
        src_ref=src,
        dst_ref=dst,
        send_sem=send,
        recv_sem=recv,
        device_id=place,
        device_id_type=pl.DeviceIdType.MESH,
    )


def front_kernel(nx, nz, mine_ref, rest_ref, top_ref, first_ref, work, upper, solved, gram_ref,
                 lhs, rhs,
                 panel_l, panel_r, part, in_f, in_s, in_z,
                 fetch_sem, swap_send, swap_recv, pair_sems, z_send, z_recv, g_send, g_recv):
    m, width = mine_ref.shape
    n = 2 * width
    whole_ref = work.at[pl.ds(n, m)]
    rows_id = lax.axis_index("rows")
    core = lax.axis_index("tensor")
    x, z = rows_id // nz, rows_id % nz
    near = x + 1 - 2 * (x % 2)
    far = nx - 1 - x
    high = x // 2
    low = (high + x % 2) % 2
    first = (1 - core) * near + core * far
    second = (1 - core) * far + core * near
    bit_f = (1 - core) * low + core * high
    bit_s = (1 - core) * high + core * low
    to_core = {"rows": rows_id, "tensor": 1 - core}
    to_first = {"rows": first * nz + z, "tensor": core}
    to_second = {"rows": second * nz + z, "tensor": core}

    def to_z(step):
        return {"rows": x * nz + (z + step) % nz, "tensor": core}

    own = pl.ds(pl.multiple_of(core * width, width), width)
    barrier = pltpu.get_barrier_semaphore()
    places = [to_core, to_first, to_second] + [to_z(s) for s in range(1, nz)]
    for place in places:
        pl.semaphore_signal(
            barrier, inc=1, device_id=place, device_id_type=pl.DeviceIdType.MESH
        )
    pieces = width // BLOCK
    fetch = pltpu.make_async_copy(mine_ref, whole_ref.at[:, own], fetch_sem)
    fetch.start()
    upper[...] = jnp.zeros(upper.shape, f32)
    fetch.wait()

    def columns(side, piece):
        return pl.ds(pl.multiple_of(side * width + piece * BLOCK, BLOCK), BLOCK)

    def prepare(side, piece):
        at = columns(side, piece)
        parts = split3(whole_ref[:, at].T)
        lhs[at] = left(parts, 1)
        rhs[at] = right(parts, 1)

    def swap(side, piece):
        view = whole_ref.at[:, columns(side, piece)]
        return remote(view, view, swap_send.at[piece], swap_recv.at[piece], to_core)

    for c in range(pieces):
        prepare(core, c)
    pl.semaphore_wait(barrier, len(places))
    for c in range(pieces):
        swap(core, c).start()

    def stage_swap(c):
        swap(core, c).wait_send()
        swap(1 - core, c).wait_recv()
        prepare(1 - core, c)

    blocks = lower_blocks(2 * width // BLOCK)
    starts = [sum(CHUNK_BLOCKS[:i]) for i in range(len(CHUNK_BLOCKS) + 1)]

    def span(ref, start, rows):
        return ref.at[pl.ds(pl.multiple_of(start, 8), rows)]

    def half(i, ref, at, which):
        rows = CHUNK_BLOCKS[i] * BLOCK // 2
        return span(ref, at + rows * which, rows)

    def quarter(i, ref, at, which):
        rows = CHUNK_BLOCKS[i] * BLOCK // 4
        return span(ref, at + rows * which, rows)

    def piece(i, ref, at, index):
        rows = CHUNK_BLOCKS[i] * BLOCK // (nx * nz)
        return span(ref, at + rows * index, rows)

    def part_of(i):
        return starts[i] * BLOCK

    def gram_of(i, side):
        return (2 * starts[i] + side * CHUNK_BLOCKS[i]) * BLOCK

    def copy_first(i):
        return remote(
            half(i, part, part_of(i), 1 - bit_f), half(i, in_f, part_of(i) // 2, 0),
            pair_sems.at[i, 0], pair_sems.at[i, 1], to_first)

    def copy_second(i):
        return remote(
            quarter(i, part, part_of(i), 2 * bit_f + 1 - bit_s),
            quarter(i, in_s, part_of(i) // 4, 0),
            pair_sems.at[i, 2], pair_sems.at[i, 3], to_second)

    def own_part(i):
        return part_of(i) + (2 * bit_f + bit_s) * (CHUNK_BLOCKS[i] * BLOCK // 4)

    def own_gram(i):
        return gram_of(i, core) + (2 * bit_f + bit_s) * (CHUNK_BLOCKS[i] * BLOCK // 4)

    def in_piece(i, index):
        return piece(i, in_z, part_of(i) // nx, index)

    def copy_z(i, step):
        return remote(
            piece(i, part, own_part(i), (z + step) % nz), in_piece(i, nz - step),
            z_send.at[i, step], z_recv.at[i, nz - step], to_z(step))

    def copy_z_in(i, step):
        return remote(
            piece(i, part, own_part(i), z), in_piece(i, step),
            z_send.at[i, step], z_recv.at[i, step], to_z(step))

    def copy_gather(i, step):
        mine = piece(i, gram_ref, own_gram(i), z)
        return remote(mine, mine, g_send.at[i, step], g_recv.at[i, nz - step], to_z(step))

    def copy_gather_in(i, step):
        theirs = piece(i, gram_ref, own_gram(i), (z + step) % nz)
        return remote(theirs, theirs, g_send.at[i, step], g_recv.at[i, step], to_z(step))

    def copy_back_second(i, bit):
        view = quarter(i, gram_ref, gram_of(i, core), 2 * bit_f + bit)
        return remote(view, view, pair_sems.at[i, 4], pair_sems.at[i, 5], to_second)

    def copy_back_first(i, bit):
        view = half(i, gram_ref, gram_of(i, core), bit)
        return remote(view, view, pair_sems.at[i, 6], pair_sems.at[i, 7], to_first)

    def copy_core(i, side):
        view = span(gram_ref, gram_of(i, side), CHUNK_BLOCKS[i] * BLOCK)
        return remote(view, view, pair_sems.at[i, 8], pair_sems.at[i, 9], to_core)

    def stage_gram(i):
        for q in range(CHUNK_BLOCKS[i]):
            a, b = blocks[2 * starts[i] + q], blocks[2 * starts[i] + CHUNK_BLOCKS[i] + q]
            bi = pl.multiple_of((a[0] + core * (b[0] - a[0])) * BLOCK, BLOCK)
            bj = pl.multiple_of((a[1] + core * (b[1] - a[1])) * BLOCK, BLOCK)
            at = (starts[i] + q) * BLOCK
            part[at : at + BLOCK] = dot_over(lhs[pl.ds(bi, BLOCK)], rhs[pl.ds(bj, BLOCK)], 1)

    def stage_send(i):
        copy_first(i).start()

    def stage_first(i):
        copy_first(i).wait()
        half(i, part, part_of(i), bit_f)[...] += half(i, in_f, part_of(i) // 2, 0)[...]
        copy_second(i).start()

    def stage_second(i):
        copy_second(i).wait()
        mine = quarter(i, part, own_part(i), 0)
        mine[...] += quarter(i, in_s, part_of(i) // 4, 0)[...]
        for step in range(1, nz):
            copy_z(i, step).start()

    def stage_scatter(i):
        total = piece(i, part, own_part(i), z)[...]
        for step in range(1, nz):
            copy_z_in(i, step).wait_recv()
            total = total + in_piece(i, step)[...]
        piece(i, gram_ref, own_gram(i), z)[...] = total
        for step in range(1, nz):
            copy_gather(i, step).start()

    def stage_gather(i):
        for step in range(1, nz):
            copy_gather_in(i, step).wait_recv()
        copy_back_second(i, bit_s).start()

    def stage_back_second(i):
        copy_back_second(i, 1 - bit_s).wait_recv()
        copy_back_first(i, bit_f).start()

    def stage_back_first(i):
        copy_back_first(i, 1 - bit_f).wait_recv()
        copy_core(i, core).start()

    def stage_core(i):
        copy_core(i, 1 - core).wait_recv()

    def stage_add(i):
        for at in range(2 * starts[i], 2 * starts[i + 1]):
            bi, bj = blocks[at]
            to = slice(bi * BLOCK, (bi + 1) * BLOCK), slice(bj * BLOCK, (bj + 1) * BLOCK)
            block = gram_ref[at * BLOCK : (at + 1) * BLOCK]
            if bj == 0:
                work[to] = block
            else:
                work[to] += block

    stages = dict(
        P=stage_swap, G=stage_gram, F=stage_send, S=stage_first, Z=stage_second, A=stage_scatter,
        B=stage_gather, C=stage_back_second, D=stage_back_first, E=stage_core, W=stage_add)
    todo = stage_order()

    def run(count, updated):
        while todo and count:
            name, i = todo[0]
            if name == "W" and i > 0 and not updated:
                return
            todo.pop(0)
            stages[name](i)
            count -= 1

    def put_upper(row, col, block):
        upper[row : row + BLOCK, col : col + BLOCK] = block

    def put_solved(row, col, block):
        solved[row : row + BLOCK, col : col + BLOCK] = block

    chunks = len(CHUNK_BLOCKS)
    middle = upper.shape[0]
    for at in factor_steps(work, panel_l, panel_r, n, 0, 0, middle, put_upper, put_solved):
        if at is not None:
            c0 = at
            need = max(i for i in range(chunks) if blocks[2 * starts[i]][1] * BLOCK <= c0)
            while ("W", need) in todo:
                run(1, c0 > 0)
        else:
            run(PACE, c0 > 0)
    run(len(todo), True)
    scale = jnp.sqrt(jnp.float32(m * nx * nz))
    top_ref[...] = upper[:, own] / scale
    first_ref[...] = solved[:, own] * scale
    rest_ref[...] = work[middle:, middle:]
    for i in range(chunks):
        for step in range(1, nz):
            copy_z(i, step).wait_send()
            copy_gather(i, step).wait_send()
        copy_back_second(i, bit_s).wait_send()
        copy_back_first(i, bit_f).wait_send()
        copy_core(i, core).wait_send()


def front(mine, nx, nz):
    m, width = mine.shape
    n = 2 * width
    middle = FRONT_STEPS * BLOCK
    count = len(lower_blocks(n // BLOCK))
    chunks = len(CHUNK_BLOCKS)
    dma = pltpu.SemaphoreType.DMA
    return pl.pallas_call(
        functools.partial(front_kernel, nx, nz),
        out_shape=[
            jax.ShapeDtypeStruct((n + m - middle, n - middle), f32),
            jax.ShapeDtypeStruct((middle, width), f32),
            jax.ShapeDtypeStruct((m, width), f32),
        ],
        in_specs=[pl.BlockSpec(memory_space=pltpu.HBM)],
        out_specs=[pl.BlockSpec(memory_space=pltpu.VMEM)] * 3,
        scratch_shapes=[
            pltpu.VMEM((n + m, n), f32),
            pltpu.VMEM((middle, n), f32),
            pltpu.VMEM((m, n), f32),
            pltpu.VMEM((count * BLOCK, BLOCK), f32),
            pltpu.VMEM((n, 6 * m), bf16),
            pltpu.VMEM((n, 6 * m), bf16),
            pltpu.VMEM((n + m, 6 * BLOCK), bf16),
            pltpu.VMEM((n, 6 * BLOCK), bf16),
            pltpu.VMEM((count * BLOCK // 2, BLOCK), f32),
            pltpu.VMEM((count * BLOCK // 4, BLOCK), f32),
            pltpu.VMEM((count * BLOCK // 8, BLOCK), f32),
            pltpu.VMEM((count * BLOCK // (2 * nx), BLOCK), f32),
            dma(()),
            dma((4,)),
            dma((4,)),
            dma((chunks, 10)),
            dma((chunks, nz)),
            dma((chunks, nz)),
            dma((chunks, nz)),
            dma((chunks, nz)),
        ],
        compiler_params=pltpu.CompilerParams(
            collective_id=0, has_side_effects=True, vmem_limit_bytes=40 * 2**20
        ),
    )(mine)


def back_kernel(total, rest_ref, top_ref, first_ref, basis_ref, triangle_ref, work, lhs, rhs):
    core = lax.axis_index("tensor")
    base = top_ref.shape[0]
    n, width = triangle_ref.shape
    scale = jnp.sqrt(jnp.float32(total))
    work[...] = rest_ref[...]
    triangle_ref[:base] = top_ref[...]
    triangle_ref[base:] = jnp.zeros((n - base, width), f32)

    basis_ref[...] = first_ref[...]

    def put_upper(row, col, block):
        at = slice(row, row + BLOCK), slice(col - width, col - width + BLOCK)
        triangle_ref[at] = jnp.where(core == 1, block / scale, 0.0)

    def put_solved(row, col, block):
        at = slice(row, row + BLOCK), slice(col - width, col - width + BLOCK)
        basis_ref[at] = jnp.where(core == 1, block * scale, basis_ref[at])

    for _ in factor_steps(work, lhs, rhs, n, base, base, n, put_upper, put_solved):
        pass


def back(rest, top, first, total):
    m, width = first.shape
    n = 2 * width
    middle = top.shape[0]
    return pl.pallas_call(
        functools.partial(back_kernel, total),
        out_shape=[
            jax.ShapeDtypeStruct((m, width), f32),
            jax.ShapeDtypeStruct((n, width), f32),
        ],
        scratch_shapes=[
            pltpu.VMEM(rest.shape, f32),
            pltpu.VMEM((rest.shape[0], 6 * BLOCK), bf16),
            pltpu.VMEM((n - middle, 6 * BLOCK), bf16),
        ],
        compiler_params=pltpu.CompilerParams(vmem_limit_bytes=30 * 2**20),
    )(rest, top, first)


def shards(effects):
    nx, nz = 4, lax.axis_size("rows") // 4
    total = effects.shape[0] * lax.axis_size("rows")
    rest, top, first = front(effects, nx, nz)
    return tuple(back(rest, top, first, total))


def solution(mesh):
    in_specs = (P(("groups", "rows"), "tensor"),)
    out_specs = (P(("groups", "rows"), "tensor"), P("groups", "tensor"))
    return jax.shard_map(shards, mesh=mesh, in_specs=in_specs, out_specs=out_specs, check_vma=False)
```

```python
import functools

import jax
import jax.numpy as jnp
from jax import lax
from jax.experimental import pallas as pl
from jax.experimental.pallas import tpu as pltpu
from jax.sharding import PartitionSpec as P

f32 = jnp.float32
bf16 = jnp.bfloat16
BLOCK = 128
BASE = 32


def split3(x):
    high = x.astype(bf16)
    rest = x - high.astype(f32)
    middle = rest.astype(bf16)
    return high, middle, (rest - middle.astype(f32)).astype(bf16)


def left(parts, dim):
    h, m, l = parts
    return jnp.concatenate([h, h, m, h, m, l], dim)


def right(parts, dim):
    h, m, l = parts
    return jnp.concatenate([h, m, h, l, m, h], dim)


def dot_over(a, b, dim):
    return lax.dot_general(a, b, (((dim,), (dim,)), ((), ())), preferred_element_type=f32)


def eliminate(rows, offset):
    tiles = BASE // 8
    cols = [
        [
            jnp.broadcast_to(rows[8 * t : 8 * t + 8, offset + j : offset + j + 1], (8, BLOCK))
            for t in range(tiles)
        ]
        for j in range(BASE)
    ]
    panel = [
        [rows[8 * t : 8 * t + 8, BLOCK * c : BLOCK * (c + 1)] for c in range(2)]
        for t in range(tiles)
    ]
    row = lax.broadcasted_iota(jnp.int32, (8, BLOCK), 0)
    scales = [jnp.zeros((8, BLOCK), f32) for _ in range(tiles)]
    for j in range(BASE):
        t0, r = divmod(j, 8)
        inv = lax.rsqrt(jnp.broadcast_to(cols[j][t0][r : r + 1], (8, BLOCK)))
        scales[t0] = jnp.where(row == r, inv, scales[t0])
        column = [cols[j][t] * inv for t in range(t0, tiles)]
        below = [jnp.where(row > r, column[0], 0.0)] + column[1:]
        pivot = [jnp.broadcast_to(panel[t0][c][r : r + 1], (8, BLOCK)) * inv for c in range(2)]
        for t in range(t0, tiles):
            for c in range(2):
                panel[t][c] = panel[t][c] - below[t - t0] * pivot[c]
        for j2 in range(j + 1, BASE):
            t2, r2 = divmod(j2, 8)
            factor = jnp.broadcast_to(column[t2 - t0][r2 : r2 + 1], (8, BLOCK))
            for t in range(t2, tiles):
                cols[j2][t] = cols[j2][t] - column[t - t0] * factor
    return jnp.concatenate(
        [jnp.concatenate([panel[t][c] * scales[t] for c in range(2)], 1) for t in range(tiles)], 0
    )


def factor_block(block, beside):
    shape = (BLOCK, BLOCK)
    row = lax.broadcasted_iota(jnp.int32, shape, 0)
    col = lax.broadcasted_iota(jnp.int32, shape, 1)
    rest = jnp.concatenate([block, jnp.where(row == col, 1.0, 0.0).astype(f32)], 1)
    done = []
    parts = BLOCK // BASE
    for p in range(parts):
        s = p * BASE
        for call in beside[len(beside) * p // parts : len(beside) * (p + 1) // parts]:
            call()
        rows = eliminate(rest[:BASE], s)
        at = lax.broadcasted_iota(jnp.int32, rows.shape, 1)
        diag = lax.broadcasted_iota(jnp.int32, rows.shape, 0) + s
        rows = jnp.where(at < jnp.minimum(diag, BLOCK), 0.0, rows)
        done.append(rows)
        if s + BASE < BLOCK:
            update = dot_over(left(split3(rows[:, :BLOCK]), 0), right(split3(rows), 0), 0)
            rest = rest[BASE:] - update[s + BASE :]
        yield
    return jnp.concatenate(done, 0)


def factor_steps(work, lhs, rhs, n, base, first, last, put_upper, put_solved):
    full = work.shape[0] + base

    def update(r, h, j, w):
        at = slice(r - base, r - base + h), slice(j - base, j - base + w)
        work[at] -= dot_over(lhs[at[0]], rhs[at[1]], 1)

    beside = []
    for c0 in range(first, last, BLOCK):
        yield c0
        c1 = c0 + BLOCK
        cols = slice(c0 - base, c1 - base)
        factored = yield from factor_block(work[cols, cols], beside)
        put_upper(c0, c0, factored[:, :BLOCK])
        inverse = right(split3(factored[:, BLOCK:]), 1)
        for r in range(c1, full, BLOCK):
            at = slice(r - base, r - base + BLOCK)
            solved = dot_over(left(split3(work[at, cols]), 1), inverse, 1)
            parts = split3(solved)
            lhs[at] = left(parts, 1)
            if r >= n:
                put_solved(r - n, c0, solved)
            else:
                put_upper(c0, r, solved.T)
                rhs[at] = right(parts, 1)
        yield
        beside = []
        j = c1
        while j < n:
            width = BLOCK if (j // BLOCK) % 2 else min(2 * BLOCK, n - j)
            top = j
            if j == c1:
                update(j, BLOCK, j, BLOCK)
                if width > BLOCK:
                    beside.append(functools.partial(update, j, BLOCK, j + BLOCK, BLOCK))
                top = j + BLOCK
            for r in range(top, full, 2 * BLOCK):
                h = min(2 * BLOCK, full - r)
                beside.append(functools.partial(update, r, h, j, width))
            j += width
    for call in beside:
        call()


CHUNK_BLOCKS = (4, 4, 4, 4, 2)
CHUNK_STARTS = (0, 2, 4, 6, 8)
STAGE_TIMES = (
    ("S", 2.9, 0.37),
    ("Z", 2.0, 0.18),
    ("A", 2.8, 0.4),
    ("B", 4.6, 0.4),
    ("C", 3.1, 0.18),
    ("D", 2.6, 0.37),
    ("E", 1.2, 0.1),
    ("W", 0.1, 0.0),
)
FRONT_STEPS = 6
PACE = 1


def stage_order():
    timed = [(0.0, 1, "P", c) for c in range(4)]
    for i, (start, n) in enumerate(zip(CHUNK_STARTS, CHUNK_BLOCKS)):
        timed.append((start - 1.0, 2 if i else 0, "G", i))
        timed.append((start - 1.0 if i == 0 else start, 3 if i else 0, "F", i))
        at = start
        for name, fixed, each in STAGE_TIMES:
            at += fixed + each * n
            timed.append((at, 4 + i, name, i))
    first = [("P", 0)]
    return first + [e[2:] for e in sorted(timed, key=lambda e: e[:2]) if e[2:] != first[0]]


def lower_blocks(count):
    return [(i, j) for j in range(count) for i in range(j, count)]


def remote(src, dst, send, recv, place):
    return pltpu.make_async_remote_copy(
        src_ref=src,
        dst_ref=dst,
        send_sem=send,
        recv_sem=recv,
        device_id=place,
        device_id_type=pl.DeviceIdType.MESH,
    )


def front_kernel(nx, nz, mine_ref, rest_ref, top_ref, first_ref, work, upper, solved, gram_ref,
                 lhs, rhs,
                 panel_l, panel_r, part, in_f, in_s, in_z,
                 fetch_sem, swap_send, swap_recv, pair_sems, z_send, z_recv, g_send, g_recv):
    m, width = mine_ref.shape
    n = 2 * width
    whole_ref = work.at[pl.ds(n, m)]
    rows_id = lax.axis_index("rows")
    core = lax.axis_index("tensor")
    x, z = rows_id // nz, rows_id % nz
    near = x + 1 - 2 * (x % 2)
    far = nx - 1 - x
    high = x // 2
    low = (high + x % 2) % 2
    first = (1 - core) * near + core * far
    second = (1 - core) * far + core * near
    bit_f = (1 - core) * low + core * high
    bit_s = (1 - core) * high + core * low
    to_core = {"rows": rows_id, "tensor": 1 - core}
    to_first = {"rows": first * nz + z, "tensor": core}
    to_second = {"rows": second * nz + z, "tensor": core}

    def to_z(step):
        return {"rows": x * nz + (z + step) % nz, "tensor": core}

    own = pl.ds(pl.multiple_of(core * width, width), width)
    barrier = pltpu.get_barrier_semaphore()
    places = [to_core, to_first, to_second] + [to_z(s) for s in range(1, nz)]
    for place in places:
        pl.semaphore_signal(
            barrier, inc=1, device_id=place, device_id_type=pl.DeviceIdType.MESH
        )
    pieces = width // BLOCK
    fetch = pltpu.make_async_copy(mine_ref, whole_ref.at[:, own], fetch_sem)
    fetch.start()
    upper[...] = jnp.zeros(upper.shape, f32)
    work[:n] = jnp.zeros((n, n), f32)
    fetch.wait()

    def columns(side, piece):
        return pl.ds(pl.multiple_of(side * width + piece * BLOCK, BLOCK), BLOCK)

    def prepare(side, piece):
        at = columns(side, piece)
        parts = split3(whole_ref[:, at].T)
        lhs[at] = left(parts, 1)
        rhs[at] = right(parts, 1)

    def swap(side, piece):
        view = whole_ref.at[:, columns(side, piece)]
        return remote(view, view, swap_send.at[piece], swap_recv.at[piece], to_core)

    for c in range(pieces):
        prepare(core, c)
    pl.semaphore_wait(barrier, len(places))
    for c in range(pieces):
        swap(core, c).start()

    def stage_swap(c):
        swap(core, c).wait_send()
        swap(1 - core, c).wait_recv()
        prepare(1 - core, c)

    blocks = lower_blocks(2 * width // BLOCK)
    starts = [sum(CHUNK_BLOCKS[:i]) for i in range(len(CHUNK_BLOCKS) + 1)]

    def span(ref, start, rows):
        return ref.at[pl.ds(pl.multiple_of(start, 8), rows)]

    def half(i, ref, at, which):
        rows = CHUNK_BLOCKS[i] * BLOCK // 2
        return span(ref, at + rows * which, rows)

    def quarter(i, ref, at, which):
        rows = CHUNK_BLOCKS[i] * BLOCK // 4
        return span(ref, at + rows * which, rows)

    def piece(i, ref, at, index):
        rows = CHUNK_BLOCKS[i] * BLOCK // (nx * nz)
        return span(ref, at + rows * index, rows)

    def part_of(i):
        return starts[i] * BLOCK

    def gram_of(i, side):
        return (2 * starts[i] + side * CHUNK_BLOCKS[i]) * BLOCK

    def copy_first(i):
        return remote(
            half(i, part, part_of(i), 1 - bit_f), half(i, in_f, part_of(i) // 2, 0),
            pair_sems.at[i, 0], pair_sems.at[i, 1], to_first)

    def copy_second(i):
        return remote(
            quarter(i, part, part_of(i), 2 * bit_f + 1 - bit_s),
            quarter(i, in_s, part_of(i) // 4, 0),
            pair_sems.at[i, 2], pair_sems.at[i, 3], to_second)

    def own_part(i):
        return part_of(i) + (2 * bit_f + bit_s) * (CHUNK_BLOCKS[i] * BLOCK // 4)

    def own_gram(i):
        return gram_of(i, core) + (2 * bit_f + bit_s) * (CHUNK_BLOCKS[i] * BLOCK // 4)

    def in_piece(i, index):
        return piece(i, in_z, part_of(i) // nx, index)

    def copy_z(i, step):
        return remote(
            piece(i, part, own_part(i), (z + step) % nz), in_piece(i, nz - step),
            z_send.at[i, step], z_recv.at[i, nz - step], to_z(step))

    def copy_z_in(i, step):
        return remote(
            piece(i, part, own_part(i), z), in_piece(i, step),
            z_send.at[i, step], z_recv.at[i, step], to_z(step))

    def copy_gather(i, step):
        mine = piece(i, gram_ref, own_gram(i), z)
        return remote(mine, mine, g_send.at[i, step], g_recv.at[i, nz - step], to_z(step))

    def copy_gather_in(i, step):
        theirs = piece(i, gram_ref, own_gram(i), (z + step) % nz)
        return remote(theirs, theirs, g_send.at[i, step], g_recv.at[i, step], to_z(step))

    def copy_back_second(i, bit):
        view = quarter(i, gram_ref, gram_of(i, core), 2 * bit_f + bit)
        return remote(view, view, pair_sems.at[i, 4], pair_sems.at[i, 5], to_second)

    def copy_back_first(i, bit):
        view = half(i, gram_ref, gram_of(i, core), bit)
        return remote(view, view, pair_sems.at[i, 6], pair_sems.at[i, 7], to_first)

    def copy_core(i, side):
        view = span(gram_ref, gram_of(i, side), CHUNK_BLOCKS[i] * BLOCK)
        return remote(view, view, pair_sems.at[i, 8], pair_sems.at[i, 9], to_core)

    def stage_gram(i):
        for q in range(CHUNK_BLOCKS[i]):
            a, b = blocks[2 * starts[i] + q], blocks[2 * starts[i] + CHUNK_BLOCKS[i] + q]
            bi = pl.multiple_of((a[0] + core * (b[0] - a[0])) * BLOCK, BLOCK)
            bj = pl.multiple_of((a[1] + core * (b[1] - a[1])) * BLOCK, BLOCK)
            at = (starts[i] + q) * BLOCK
            part[at : at + BLOCK] = dot_over(lhs[pl.ds(bi, BLOCK)], rhs[pl.ds(bj, BLOCK)], 1)

    def stage_send(i):
        copy_first(i).start()

    def stage_first(i):
        copy_first(i).wait()
        half(i, part, part_of(i), bit_f)[...] += half(i, in_f, part_of(i) // 2, 0)[...]
        copy_second(i).start()

    def stage_second(i):
        copy_second(i).wait()
        mine = quarter(i, part, own_part(i), 0)
        mine[...] += quarter(i, in_s, part_of(i) // 4, 0)[...]
        for step in range(1, nz):
            copy_z(i, step).start()

    def stage_scatter(i):
        total = piece(i, part, own_part(i), z)[...]
        for step in range(1, nz):
            copy_z_in(i, step).wait_recv()
            total = total + in_piece(i, step)[...]
        piece(i, gram_ref, own_gram(i), z)[...] = total
        for step in range(1, nz):
            copy_gather(i, step).start()

    def stage_gather(i):
        for step in range(1, nz):
            copy_gather_in(i, step).wait_recv()
        copy_back_second(i, bit_s).start()

    def stage_back_second(i):
        copy_back_second(i, 1 - bit_s).wait_recv()
        copy_back_first(i, bit_f).start()

    def stage_back_first(i):
        copy_back_first(i, 1 - bit_f).wait_recv()
        copy_core(i, core).start()

    def stage_core(i):
        copy_core(i, 1 - core).wait_recv()

    def stage_add(i):
        for at in range(2 * starts[i], 2 * starts[i + 1]):
            bi, bj = blocks[at]
            to = slice(bi * BLOCK, (bi + 1) * BLOCK), slice(bj * BLOCK, (bj + 1) * BLOCK)
            block = gram_ref[at * BLOCK : (at + 1) * BLOCK]
            work[to] += block

    stages = dict(
        P=stage_swap, G=stage_gram, F=stage_send, S=stage_first, Z=stage_second, A=stage_scatter,
        B=stage_gather, C=stage_back_second, D=stage_back_first, E=stage_core, W=stage_add)
    todo = stage_order()

    def run(count):
        while todo and count:
            name, i = todo.pop(0)
            stages[name](i)
            count -= 1

    def put_upper(row, col, block):
        upper[row : row + BLOCK, col : col + BLOCK] = block

    def put_solved(row, col, block):
        solved[row : row + BLOCK, col : col + BLOCK] = block

    chunks = len(CHUNK_BLOCKS)
    middle = upper.shape[0]
    for at in factor_steps(work, panel_l, panel_r, n, 0, 0, middle, put_upper, put_solved):
        if at is not None:
            c0 = at
            need = max(i for i in range(chunks) if blocks[2 * starts[i]][1] * BLOCK <= c0)
            while ("W", need) in todo:
                run(1)
        else:
            run(PACE)
    run(len(todo))
    scale = jnp.sqrt(jnp.float32(m * nx * nz))
    top_ref[...] = upper[:, own] / scale
    first_ref[...] = solved[:, own] * scale
    rest_ref[...] = work[middle:, middle:]
    for i in range(chunks):
        for step in range(1, nz):
            copy_z(i, step).wait_send()
            copy_gather(i, step).wait_send()
        copy_back_second(i, bit_s).wait_send()
        copy_back_first(i, bit_f).wait_send()
        copy_core(i, core).wait_send()


def front(mine, nx, nz):
    m, width = mine.shape
    n = 2 * width
    middle = FRONT_STEPS * BLOCK
    count = len(lower_blocks(n // BLOCK))
    chunks = len(CHUNK_BLOCKS)
    dma = pltpu.SemaphoreType.DMA
    return pl.pallas_call(
        functools.partial(front_kernel, nx, nz),
        out_shape=[
            jax.ShapeDtypeStruct((n + m - middle, n - middle), f32),
            jax.ShapeDtypeStruct((middle, width), f32),
            jax.ShapeDtypeStruct((m, width), f32),
        ],
        in_specs=[pl.BlockSpec(memory_space=pltpu.HBM)],
        out_specs=[pl.BlockSpec(memory_space=pltpu.VMEM)] * 3,
        scratch_shapes=[
            pltpu.VMEM((n + m, n), f32),
            pltpu.VMEM((middle, n), f32),
            pltpu.VMEM((m, n), f32),
            pltpu.VMEM((count * BLOCK, BLOCK), f32),
            pltpu.VMEM((n, 6 * m), bf16),
            pltpu.VMEM((n, 6 * m), bf16),
            pltpu.VMEM((n + m, 6 * BLOCK), bf16),
            pltpu.VMEM((n, 6 * BLOCK), bf16),
            pltpu.VMEM((count * BLOCK // 2, BLOCK), f32),
            pltpu.VMEM((count * BLOCK // 4, BLOCK), f32),
            pltpu.VMEM((count * BLOCK // 8, BLOCK), f32),
            pltpu.VMEM((count * BLOCK // (2 * nx), BLOCK), f32),
            dma(()),
            dma((4,)),
            dma((4,)),
            dma((chunks, 10)),
            dma((chunks, nz)),
            dma((chunks, nz)),
            dma((chunks, nz)),
            dma((chunks, nz)),
        ],
        compiler_params=pltpu.CompilerParams(
            collective_id=0, has_side_effects=True, vmem_limit_bytes=40 * 2**20
        ),
    )(mine)


def back_kernel(total, rest_ref, top_ref, first_ref, basis_ref, triangle_ref, work, lhs, rhs,
                bottom, sems):
    core = lax.axis_index("tensor")
    base = top_ref.shape[0]
    n, width = triangle_ref.shape
    scale = jnp.sqrt(jnp.float32(total))
    work[...] = rest_ref[...]
    put_top = pltpu.make_async_copy(top_ref, triangle_ref.at[pl.ds(0, base)], sems.at[0])
    put_top.start()
    bottom[...] = jnp.zeros(bottom.shape, f32)

    basis_ref[...] = first_ref[...]

    def put_upper(row, col, block):
        at = slice(row - base, row - base + BLOCK), slice(col - width, col - width + BLOCK)
        bottom[at] = jnp.where(core == 1, block / scale, 0.0)

    def put_solved(row, col, block):
        at = slice(row, row + BLOCK), slice(col - width, col - width + BLOCK)
        basis_ref[at] = jnp.where(core == 1, block * scale, basis_ref[at])

    for _ in factor_steps(work, lhs, rhs, n, base, base, n, put_upper, put_solved):
        pass
    put_bottom = pltpu.make_async_copy(
        bottom, triangle_ref.at[pl.ds(base, n - base)], sems.at[1]
    )
    put_bottom.start()
    put_bottom.wait()
    put_top.wait()


def back(rest, top, first, total):
    m, width = first.shape
    n = 2 * width
    middle = top.shape[0]
    return pl.pallas_call(
        functools.partial(back_kernel, total),
        out_shape=[
            jax.ShapeDtypeStruct((m, width), f32),
            jax.ShapeDtypeStruct((n, width), f32),
        ],
        scratch_shapes=[
            pltpu.VMEM(rest.shape, f32),
            pltpu.VMEM((rest.shape[0], 6 * BLOCK), bf16),
            pltpu.VMEM((n - middle, 6 * BLOCK), bf16),
            pltpu.VMEM((n - middle, width), f32),
            pltpu.SemaphoreType.DMA((2,)),
        ],
        out_specs=[
            pl.BlockSpec(memory_space=pltpu.VMEM),
            pl.BlockSpec(memory_space=pltpu.HBM),
        ],
        compiler_params=pltpu.CompilerParams(vmem_limit_bytes=30 * 2**20),
    )(rest, top, first)


def shards(effects):
    nx, nz = 4, lax.axis_size("rows") // 4
    total = effects.shape[0] * lax.axis_size("rows")
    rest, top, first = front(effects, nx, nz)
    return tuple(back(rest, top, first, total))


def solution(mesh):
    in_specs = (P(("groups", "rows"), "tensor"),)
    out_specs = (P(("groups", "rows"), "tensor"), P("groups", "tensor"))
    return jax.shard_map(shards, mesh=mesh, in_specs=in_specs, out_specs=out_specs, check_vma=False)
```

```python
import functools

import jax
import jax.numpy as jnp
from jax import lax
from jax.experimental import pallas as pl
from jax.experimental.pallas import tpu as pltpu
from jax.sharding import PartitionSpec as P

f32 = jnp.float32
bf16 = jnp.bfloat16
BLOCK = 128
BASE = 32


def split3(x):
    high = x.astype(bf16)
    rest = x - high.astype(f32)
    middle = rest.astype(bf16)
    return high, middle, (rest - middle.astype(f32)).astype(bf16)


def left(parts, dim):
    h, m, l = parts
    return jnp.concatenate([h, h, m, h, m, l], dim)


def right(parts, dim):
    h, m, l = parts
    return jnp.concatenate([h, m, h, l, m, h], dim)


def dot_over(a, b, dim):
    return lax.dot_general(a, b, (((dim,), (dim,)), ((), ())), preferred_element_type=f32)


def eliminate(rows, offset):
    tiles = BASE // 8
    cols = [
        [
            jnp.broadcast_to(rows[8 * t : 8 * t + 8, offset + j : offset + j + 1], (8, BLOCK))
            for t in range(tiles)
        ]
        for j in range(BASE)
    ]
    panel = [
        [rows[8 * t : 8 * t + 8, BLOCK * c : BLOCK * (c + 1)] for c in range(2)]
        for t in range(tiles)
    ]
    row = lax.broadcasted_iota(jnp.int32, (8, BLOCK), 0)
    scales = [jnp.zeros((8, BLOCK), f32) for _ in range(tiles)]
    for j in range(BASE):
        t0, r = divmod(j, 8)
        inv = lax.rsqrt(jnp.broadcast_to(cols[j][t0][r : r + 1], (8, BLOCK)))
        scales[t0] = jnp.where(row == r, inv, scales[t0])
        column = [cols[j][t] * inv for t in range(t0, tiles)]
        below = [jnp.where(row > r, column[0], 0.0)] + column[1:]
        pivot = [jnp.broadcast_to(panel[t0][c][r : r + 1], (8, BLOCK)) * inv for c in range(2)]
        for t in range(t0, tiles):
            for c in range(2):
                panel[t][c] = panel[t][c] - below[t - t0] * pivot[c]
        for j2 in range(j + 1, BASE):
            t2, r2 = divmod(j2, 8)
            factor = jnp.broadcast_to(column[t2 - t0][r2 : r2 + 1], (8, BLOCK))
            for t in range(t2, tiles):
                cols[j2][t] = cols[j2][t] - column[t - t0] * factor
    return jnp.concatenate(
        [jnp.concatenate([panel[t][c] * scales[t] for c in range(2)], 1) for t in range(tiles)], 0
    )


def factor_block(block):
    shape = (BLOCK, BLOCK)
    row = lax.broadcasted_iota(jnp.int32, shape, 0)
    col = lax.broadcasted_iota(jnp.int32, shape, 1)
    rest = jnp.concatenate([block, jnp.where(row == col, 1.0, 0.0).astype(f32)], 1)
    done = []
    for s in range(0, BLOCK, BASE):
        rows = eliminate(rest[:BASE], s)
        at = lax.broadcasted_iota(jnp.int32, rows.shape, 1)
        diag = lax.broadcasted_iota(jnp.int32, rows.shape, 0) + s
        rows = jnp.where(at < jnp.minimum(diag, BLOCK), 0.0, rows)
        done.append(rows)
        if s + BASE < BLOCK:
            update = dot_over(left(split3(rows[:, :BLOCK]), 0), right(split3(rows), 0), 0)
            rest = rest[BASE:] - update[s + BASE :]
        yield
    return jnp.concatenate(done, 0)


def factor_steps(work, lhs, rhs, n, base, first, last, put_upper, put_solved):
    full = work.shape[0] + base
    for c0 in range(first, last, BLOCK):
        yield c0
        c1 = c0 + BLOCK
        cols = slice(c0 - base, c1 - base)
        factored = yield from factor_block(work[cols, cols])
        put_upper(c0, c0, factored[:, :BLOCK])
        inverse = right(split3(factored[:, BLOCK:]), 1)
        for r in range(c1, full, BLOCK):
            at = slice(r - base, r - base + BLOCK)
            solved = dot_over(left(split3(work[at, cols]), 1), inverse, 1)
            parts = split3(solved)
            lhs[at] = left(parts, 1)
            if r >= n:
                put_solved(r - n, c0, solved)
            else:
                put_upper(c0, r, solved.T)
                rhs[at] = right(parts, 1)
        yield
        j = c1
        while j < n:
            width = BLOCK if (j // BLOCK) % 2 else min(2 * BLOCK, n - j)
            to = slice(j - base, j - base + width)
            against = rhs[to]
            spans = [(r, min(2 * BLOCK, n - r)) for r in range(j, n, 2 * BLOCK)]
            spans += [(r, min(2 * BLOCK, full - r)) for r in range(n, full, 2 * BLOCK)]
            for r, h in spans:
                at = slice(r - base, r - base + h)
                product = dot_over(lhs[at], against, 1)
                if c0 == 0 and r < n:
                    work[at, to] = -product
                else:
                    work[at, to] -= product
            j += width
            yield


CHUNK_BLOCKS = (4, 4, 4, 6)
CHUNK_STARTS = (0, 2.5, 5, 7.5)
STAGE_TIMES = (
    ("S", 2.9, 0.37),
    ("Z", 2.0, 0.18),
    ("A", 2.8, 0.4),
    ("B", 4.6, 0.4),
    ("C", 3.1, 0.18),
    ("D", 2.6, 0.37),
    ("E", 1.2, 0.1),
    ("W", 0.1, 0.0),
)
FRONT_STEPS = 6
PACE = 1


def stage_order():
    timed = [(0.0, 1, "P", c) for c in range(4)]
    for i, (start, n) in enumerate(zip(CHUNK_STARTS, CHUNK_BLOCKS)):
        timed.append((start - 1.0, 2 if i else 0, "G", i))
        timed.append((start - 1.0 if i == 0 else start, 3 if i else 0, "F", i))
        at = start
        for name, fixed, each in STAGE_TIMES:
            at += fixed + each * n
            timed.append((at, 4 + i, name, i))
    first = [("P", 0)]
    return first + [e[2:] for e in sorted(timed, key=lambda e: e[:2]) if e[2:] != first[0]]


def lower_blocks(count):
    return [(i, j) for j in range(count) for i in range(j, count)]


def remote(src, dst, send, recv, place):
    return pltpu.make_async_remote_copy(
        src_ref=src,
        dst_ref=dst,
        send_sem=send,
        recv_sem=recv,
        device_id=place,
        device_id_type=pl.DeviceIdType.MESH,
    )


def front_kernel(nx, nz, mine_ref, rest_ref, top_ref, first_ref, work, upper, solved, gram_ref,
                 lhs, rhs,
                 panel_l, panel_r, part, in_f, in_s, in_z,
                 fetch_sem, swap_send, swap_recv, pair_sems, z_send, z_recv, g_send, g_recv):
    m, width = mine_ref.shape
    n = 2 * width
    whole_ref = work.at[pl.ds(n, m)]
    rows_id = lax.axis_index("rows")
    core = lax.axis_index("tensor")
    x, z = rows_id // nz, rows_id % nz
    near = x + 1 - 2 * (x % 2)
    far = nx - 1 - x
    high = x // 2
    low = (high + x % 2) % 2
    first = (1 - core) * near + core * far
    second = (1 - core) * far + core * near
    bit_f = (1 - core) * low + core * high
    bit_s = (1 - core) * high + core * low
    to_core = {"rows": rows_id, "tensor": 1 - core}
    to_first = {"rows": first * nz + z, "tensor": core}
    to_second = {"rows": second * nz + z, "tensor": core}

    def to_z(step):
        return {"rows": x * nz + (z + step) % nz, "tensor": core}

    own = pl.ds(pl.multiple_of(core * width, width), width)
    barrier = pltpu.get_barrier_semaphore()
    places = [to_core, to_first, to_second] + [to_z(s) for s in range(1, nz)]
    for place in places:
        pl.semaphore_signal(
            barrier, inc=1, device_id=place, device_id_type=pl.DeviceIdType.MESH
        )
    pieces = width // BLOCK
    fetch = pltpu.make_async_copy(mine_ref, whole_ref.at[:, own], fetch_sem)
    fetch.start()
    upper[...] = jnp.zeros(upper.shape, f32)
    fetch.wait()

    def columns(side, piece):
        return pl.ds(pl.multiple_of(side * width + piece * BLOCK, BLOCK), BLOCK)

    def prepare(side, piece):
        at = columns(side, piece)
        parts = split3(whole_ref[:, at].T)
        lhs[at] = left(parts, 1)
        rhs[at] = right(parts, 1)

    def swap(side, piece):
        view = whole_ref.at[:, columns(side, piece)]
        return remote(view, view, swap_send.at[piece], swap_recv.at[piece], to_core)

    for c in range(pieces):
        prepare(core, c)
    pl.semaphore_wait(barrier, len(places))
    for c in range(pieces):
        swap(core, c).start()

    def stage_swap(c):
        swap(core, c).wait_send()
        swap(1 - core, c).wait_recv()
        prepare(1 - core, c)

    blocks = lower_blocks(2 * width // BLOCK)
    starts = [sum(CHUNK_BLOCKS[:i]) for i in range(len(CHUNK_BLOCKS) + 1)]

    def span(ref, start, rows):
        return ref.at[pl.ds(pl.multiple_of(start, 8), rows)]

    def half(i, ref, at, which):
        rows = CHUNK_BLOCKS[i] * BLOCK // 2
        return span(ref, at + rows * which, rows)

    def quarter(i, ref, at, which):
        rows = CHUNK_BLOCKS[i] * BLOCK // 4
        return span(ref, at + rows * which, rows)

    def piece(i, ref, at, index):
        rows = CHUNK_BLOCKS[i] * BLOCK // (nx * nz)
        return span(ref, at + rows * index, rows)

    def part_of(i):
        return starts[i] * BLOCK

    def gram_of(i, side):
        return (2 * starts[i] + side * CHUNK_BLOCKS[i]) * BLOCK

    def copy_first(i):
        return remote(
            half(i, part, part_of(i), 1 - bit_f), half(i, in_f, part_of(i) // 2, 0),
            pair_sems.at[i, 0], pair_sems.at[i, 1], to_first)

    def copy_second(i):
        return remote(
            quarter(i, part, part_of(i), 2 * bit_f + 1 - bit_s),
            quarter(i, in_s, part_of(i) // 4, 0),
            pair_sems.at[i, 2], pair_sems.at[i, 3], to_second)

    def own_part(i):
        return part_of(i) + (2 * bit_f + bit_s) * (CHUNK_BLOCKS[i] * BLOCK // 4)

    def own_gram(i):
        return gram_of(i, core) + (2 * bit_f + bit_s) * (CHUNK_BLOCKS[i] * BLOCK // 4)

    def in_piece(i, index):
        return piece(i, in_z, part_of(i) // nx, index)

    def copy_z(i, step):
        return remote(
            piece(i, part, own_part(i), (z + step) % nz), in_piece(i, nz - step),
            z_send.at[i, step], z_recv.at[i, nz - step], to_z(step))

    def copy_z_in(i, step):
        return remote(
            piece(i, part, own_part(i), z), in_piece(i, step),
            z_send.at[i, step], z_recv.at[i, step], to_z(step))

    def copy_gather(i, step):
        mine = piece(i, gram_ref, own_gram(i), z)
        return remote(mine, mine, g_send.at[i, step], g_recv.at[i, nz - step], to_z(step))

    def copy_gather_in(i, step):
        theirs = piece(i, gram_ref, own_gram(i), (z + step) % nz)
        return remote(theirs, theirs, g_send.at[i, step], g_recv.at[i, step], to_z(step))

    def copy_back_second(i, bit):
        view = quarter(i, gram_ref, gram_of(i, core), 2 * bit_f + bit)
        return remote(view, view, pair_sems.at[i, 4], pair_sems.at[i, 5], to_second)

    def copy_back_first(i, bit):
        view = half(i, gram_ref, gram_of(i, core), bit)
        return remote(view, view, pair_sems.at[i, 6], pair_sems.at[i, 7], to_first)

    def copy_core(i, side):
        view = span(gram_ref, gram_of(i, side), CHUNK_BLOCKS[i] * BLOCK)
        return remote(view, view, pair_sems.at[i, 8], pair_sems.at[i, 9], to_core)

    def stage_gram(i):
        for q in range(CHUNK_BLOCKS[i]):
            a, b = blocks[2 * starts[i] + q], blocks[2 * starts[i] + CHUNK_BLOCKS[i] + q]
            bi = pl.multiple_of((a[0] + core * (b[0] - a[0])) * BLOCK, BLOCK)
            bj = pl.multiple_of((a[1] + core * (b[1] - a[1])) * BLOCK, BLOCK)
            at = (starts[i] + q) * BLOCK
            part[at : at + BLOCK] = dot_over(lhs[pl.ds(bi, BLOCK)], rhs[pl.ds(bj, BLOCK)], 1)

    def stage_send(i):
        copy_first(i).start()

    def stage_first(i):
        copy_first(i).wait()
        half(i, part, part_of(i), bit_f)[...] += half(i, in_f, part_of(i) // 2, 0)[...]
        copy_second(i).start()

    def stage_second(i):
        copy_second(i).wait()
        mine = quarter(i, part, own_part(i), 0)
        mine[...] += quarter(i, in_s, part_of(i) // 4, 0)[...]
        for step in range(1, nz):
            copy_z(i, step).start()

    def stage_scatter(i):
        total = piece(i, part, own_part(i), z)[...]
        for step in range(1, nz):
            copy_z_in(i, step).wait_recv()
            total = total + in_piece(i, step)[...]
        piece(i, gram_ref, own_gram(i), z)[...] = total
        for step in range(1, nz):
            copy_gather(i, step).start()

    def stage_gather(i):
        for step in range(1, nz):
            copy_gather_in(i, step).wait_recv()
        copy_back_second(i, bit_s).start()

    def stage_back_second(i):
        copy_back_second(i, 1 - bit_s).wait_recv()
        copy_back_first(i, bit_f).start()

    def stage_back_first(i):
        copy_back_first(i, 1 - bit_f).wait_recv()
        copy_core(i, core).start()

    def stage_core(i):
        copy_core(i, 1 - core).wait_recv()

    def stage_add(i):
        for at in range(2 * starts[i], 2 * starts[i + 1]):
            bi, bj = blocks[at]
            to = slice(bi * BLOCK, (bi + 1) * BLOCK), slice(bj * BLOCK, (bj + 1) * BLOCK)
            block = gram_ref[at * BLOCK : (at + 1) * BLOCK]
            if bj == 0:
                work[to] = block
            else:
                work[to] += block

    stages = dict(
        P=stage_swap, G=stage_gram, F=stage_send, S=stage_first, Z=stage_second, A=stage_scatter,
        B=stage_gather, C=stage_back_second, D=stage_back_first, E=stage_core, W=stage_add)
    todo = stage_order()

    def run(count, updated):
        while todo and count:
            name, i = todo[0]
            if name == "W" and i > 0 and not updated:
                return
            todo.pop(0)
            stages[name](i)
            count -= 1

    def put_upper(row, col, block):
        upper[row : row + BLOCK, col : col + BLOCK] = block

    def put_solved(row, col, block):
        solved[row : row + BLOCK, col : col + BLOCK] = block

    chunks = len(CHUNK_BLOCKS)
    middle = upper.shape[0]
    for at in factor_steps(work, panel_l, panel_r, n, 0, 0, middle, put_upper, put_solved):
        if at is not None:
            c0 = at
            need = max(i for i in range(chunks) if blocks[2 * starts[i]][1] * BLOCK <= c0)
            while ("W", need) in todo:
                run(1, c0 > 0)
        else:
            run(PACE, c0 > 0)
    run(len(todo), True)
    scale = jnp.sqrt(jnp.float32(m * nx * nz))
    top_ref[...] = upper[:, own] / scale
    first_ref[...] = solved[:, own] * scale
    rest_ref[...] = work[middle:, middle:]
    for i in range(chunks):
        for step in range(1, nz):
            copy_z(i, step).wait_send()
            copy_gather(i, step).wait_send()
        copy_back_second(i, bit_s).wait_send()
        copy_back_first(i, bit_f).wait_send()
        copy_core(i, core).wait_send()


def front(mine, nx, nz):
    m, width = mine.shape
    n = 2 * width
    middle = FRONT_STEPS * BLOCK
    count = len(lower_blocks(n // BLOCK))
    chunks = len(CHUNK_BLOCKS)
    dma = pltpu.SemaphoreType.DMA
    return pl.pallas_call(
        functools.partial(front_kernel, nx, nz),
        out_shape=[
            jax.ShapeDtypeStruct((n + m - middle, n - middle), f32),
            jax.ShapeDtypeStruct((middle, width), f32),
            jax.ShapeDtypeStruct((m, width), f32),
        ],
        in_specs=[pl.BlockSpec(memory_space=pltpu.HBM)],
        out_specs=[pl.BlockSpec(memory_space=pltpu.VMEM)] * 3,
        scratch_shapes=[
            pltpu.VMEM((n + m, n), f32),
            pltpu.VMEM((middle, n), f32),
            pltpu.VMEM((m, n), f32),
            pltpu.VMEM((count * BLOCK, BLOCK), f32),
            pltpu.VMEM((n, 6 * m), bf16),
            pltpu.VMEM((n, 6 * m), bf16),
            pltpu.VMEM((n + m, 6 * BLOCK), bf16),
            pltpu.VMEM((n, 6 * BLOCK), bf16),
            pltpu.VMEM((count * BLOCK // 2, BLOCK), f32),
            pltpu.VMEM((count * BLOCK // 4, BLOCK), f32),
            pltpu.VMEM((count * BLOCK // 8, BLOCK), f32),
            pltpu.VMEM((count * BLOCK // (2 * nx), BLOCK), f32),
            dma(()),
            dma((4,)),
            dma((4,)),
            dma((chunks, 10)),
            dma((chunks, nz)),
            dma((chunks, nz)),
            dma((chunks, nz)),
            dma((chunks, nz)),
        ],
        compiler_params=pltpu.CompilerParams(
            collective_id=0, has_side_effects=True, vmem_limit_bytes=40 * 2**20
        ),
    )(mine)


def back_kernel(total, rest_ref, top_ref, first_ref, basis_ref, triangle_ref, work, lhs, rhs):
    core = lax.axis_index("tensor")
    base = top_ref.shape[0]
    n, width = triangle_ref.shape
    scale = jnp.sqrt(jnp.float32(total))
    work[...] = rest_ref[...]
    triangle_ref[:base] = top_ref[...]
    triangle_ref[base:] = jnp.zeros((n - base, width), f32)

    basis_ref[...] = first_ref[...]

    def put_upper(row, col, block):
        at = slice(row, row + BLOCK), slice(col - width, col - width + BLOCK)
        triangle_ref[at] = jnp.where(core == 1, block / scale, 0.0)

    def put_solved(row, col, block):
        at = slice(row, row + BLOCK), slice(col - width, col - width + BLOCK)
        basis_ref[at] = jnp.where(core == 1, block * scale, basis_ref[at])

    for _ in factor_steps(work, lhs, rhs, n, base, base, n, put_upper, put_solved):
        pass


def back(rest, top, first, total):
    m, width = first.shape
    n = 2 * width
    middle = top.shape[0]
    return pl.pallas_call(
        functools.partial(back_kernel, total),
        out_shape=[
            jax.ShapeDtypeStruct((m, width), f32),
            jax.ShapeDtypeStruct((n, width), f32),
        ],
        scratch_shapes=[
            pltpu.VMEM(rest.shape, f32),
            pltpu.VMEM((rest.shape[0], 6 * BLOCK), bf16),
            pltpu.VMEM((n - middle, 6 * BLOCK), bf16),
        ],
        compiler_params=pltpu.CompilerParams(vmem_limit_bytes=30 * 2**20),
    )(rest, top, first)


def shards(effects):
    nx, nz = 4, lax.axis_size("rows") // 4
    total = effects.shape[0] * lax.axis_size("rows")
    rest, top, first = front(effects, nx, nz)
    return tuple(back(rest, top, first, total))


def solution(mesh):
    in_specs = (P(("groups", "rows"), "tensor"),)
    out_specs = (P(("groups", "rows"), "tensor"), P("groups", "tensor"))
    return jax.shard_map(shards, mesh=mesh, in_specs=in_specs, out_specs=out_specs, check_vma=False)
```
